32 devices in a mesh: ba: 8 (over z, x), ka: 4 (over y, core).
Axes of the slice: x: 2, y: 2, z: 4, core: 2. Of those that a mesh axis runs over, the one named last changes fastest.
Arguments:
- emb_one: bfloat16 [8192, 128], P('ba'), may hold values from -8 to 8, as said below
- emb_two: bfloat16 [8192, 128], P('ba'), may hold values from -8 to 8, as said below
- prototypes: float32 [3000, 128], P('ka', 'ba'), may hold values from -6 to 6, as said below
Outputs:
- assignment_weights: float32 [8192, 3000], P('ba', 'ka')
- row_loss: float32 [8192], P('ba')
The draws below stay inside these ranges and needn't reach their ends.
Inputs may be any that keep to these rules, and one draw needn't show every extreme that they name: `prototypes`: prototype entries are finite and lie within the stated range. `emb_one`: embedding entries are finite and lie within the stated range; rows are not zero. `emb_two`: embedding entries are finite and lie within the stated range; rows are not zero.
All inputs are finite; a program needn't handle non-finite values.
Results may differ from the reference program's by a relative error of at most 0.0003.
Values sent between devices are 32-bit elements.
A program may use at most 64 MiB of HBM per device.

```python
import jax
import jax.numpy as jnp
from jax import lax

K = 3000
D = 128
REPEAT_COUNT = 3
ROWS = 8192


def shared_centers(key):
    raw = jax.random.normal(jax.random.fold_in(key, 7), (K, D), jnp.float32)
    return jnp.clip(raw, -6.0, 6.0)


def cluster_rows(key):
    return jax.random.randint(jax.random.fold_in(key, 11), (ROWS,), 0, K)


def view_draw(key, salt):
    centers = shared_centers(key)
    labels = cluster_rows(key)
    noise_key = jax.random.fold_in(key, salt)
    noise = jax.random.normal(noise_key, (ROWS, D), jnp.float32)
    values = centers[labels] + noise
    return jnp.clip(values, -8.0, 8.0).astype(jnp.bfloat16)


def draw_prototypes(key, part):
    return shared_centers(key)


def draw_emb_one(key, part):
    return view_draw(key, 21)


def draw_emb_two(key, part):
    return view_draw(key, 22)


def setup_inputs(seed: int = 0) -> dict:
    keys = jax.random.split(jax.random.key(seed), 4)
    emb_one = draw_emb_one(jax.random.fold_in(keys[3], 71), 0)
    emb_two = draw_emb_two(jax.random.fold_in(keys[3], 71), 0)
    prototypes = draw_prototypes(jax.random.fold_in(keys[3], 71), 0)
    return {"emb_one": emb_one, "emb_two": emb_two, "prototypes": prototypes}


TEMP_CODE = 0.05
TEMP_PRED = 0.1

def unit_rows(values):
    values = values.astype(jnp.float32)
    factor = lax.rsqrt(lax.optimization_barrier(jnp.sum(values * values, axis=1, keepdims=True)))
    return (values * factor).astype(jnp.bfloat16)

def balanced_normalizer(prototype_similarity):
    matrix = jnp.exp(prototype_similarity / TEMP_CODE)
    for iteration in range(REPEAT_COUNT):
        matrix = matrix / lax.optimization_barrier(jnp.sum(matrix, axis=0, keepdims=True))
        matrix = matrix / lax.optimization_barrier(jnp.sum(matrix, axis=1, keepdims=True))
    return matrix

def reference(emb_one, emb_two, prototypes):
    centers = unit_rows(prototypes)
    first_view_logits = jnp.dot(unit_rows(emb_one), centers.T, preferred_element_type=jnp.float32)
    second_view_logits = jnp.dot(unit_rows(emb_two), centers.T, preferred_element_type=jnp.float32)
    first_view_assignment = balanced_normalizer(first_view_logits)
    second_view_assignment = balanced_normalizer(second_view_logits)
    logp_one = jax.nn.log_softmax(first_view_logits / TEMP_PRED, axis=1)
    logp_two = jax.nn.log_softmax(second_view_logits / TEMP_PRED, axis=1)
    row_loss = -(lax.optimization_barrier(jnp.sum(first_view_assignment * logp_two, axis=1)) + lax.optimization_barrier(jnp.sum(second_view_assignment * logp_one, axis=1)))
    return (K * first_view_assignment, row_loss)
```

```python
import functools

import jax
import jax.numpy as jnp
from jax import lax
from jax.experimental import pallas as pl
from jax.experimental.pallas import tpu as pltpu
from jax.sharding import PartitionSpec as P

REPEAT_COUNT = 3
TEMP_CODE = 0.05
TEMP_PRED = 0.1
LANES = 128
VMEM_LIMIT = 48 * 1024 * 1024
MESH = pl.DeviceIdType.MESH


def unit(values):
    values = values.astype(jnp.float32)
    return (values * lax.rsqrt(jnp.sum(values * values, axis=1, keepdims=True))).astype(jnp.bfloat16)


def fold_rows(tile):
    return jnp.sum(tile.T, axis=0, keepdims=True)


def balance_kernel(
    nba, nka, width,
    one_ref, two_ref, proto_ref,
    unit_ref, centers_ref, scale_ref, mass_ref, loss_ref,
    units, gathered, scores, codes, dens, row_scale,
    col_out, col_in, row_out, row_in, last_out, last_in,
    gather_send, gather_recv, col_send, col_recv, row_send, row_recv, last_send, last_recv,
):
    mine_ba = lax.axis_index("ba")
    mine_ka = lax.axis_index("ka")
    rows = one_ref.shape[0]
    blocks = rows // LANES
    feat = proto_ref.shape[0]
    padded = centers_ref.shape[1]
    tiles = padded // LANES
    ba_peer = [lax.rem(mine_ba + d, nba) for d in range(nba)]
    ka_peer = [lax.rem(mine_ka + d, nka) for d in range(nka)]

    barrier = pltpu.get_barrier_semaphore()
    for d in range(1, nba):
        pl.semaphore_signal(barrier, inc=1, device_id={"ba": ba_peer[d]}, device_id_type=MESH)
    for d in range(1, nka):
        pl.semaphore_signal(barrier, inc=1, device_id={"ka": ka_peer[d]}, device_id_type=MESH)
    pl.semaphore_wait(barrier, nba + nka - 2)

    pending = []

    def send(src, dst, send_sem, recv_sem, peer):
        copy = pltpu.make_async_remote_copy(
            src_ref=src, dst_ref=dst, send_sem=send_sem, recv_sem=recv_sem,
            device_id=peer, device_id_type=MESH,
        )
        copy.start()
        pending.append(copy)
        return copy

    gathers = [
        send(proto_ref, gathered.at[mine_ba], gather_send.at[d], gather_recv.at[d], {"ba": ba_peer[d]})
        for d in range(1, nba)
    ]
    gathered[mine_ba] = proto_ref[...]

    def norm_block(b, carry):
        at = pl.ds(pl.multiple_of(b * LANES, LANES), LANES)
        units[0, at, :] = unit(one_ref[at, :])
        units[1, at, :] = unit(two_ref[at, :])
        return carry

    lax.fori_loop(0, blocks, norm_block, 0)
    for copy in gathers:
        copy.wait_recv()
    whole = jnp.concatenate([gathered[b] for b in range(nba)], axis=0)
    factor = lax.rsqrt(jnp.sum(whole * whole, axis=0, keepdims=True))
    centers_ref[...] = jnp.zeros_like(centers_ref)
    centers_ref[:, :width] = (whole * factor).astype(jnp.bfloat16)

    valid = lax.broadcasted_iota(jnp.int32, (1, padded), 1) < width

    def lane(t):
        return slice(t * LANES, (t + 1) * LANES)

    def to_sublanes(acc):
        return jnp.concatenate([jnp.sum(a, axis=0, keepdims=True) for a in acc], axis=1)

    def fold8(tile):
        return jnp.sum(tile.reshape(LANES // 8, 8, LANES), axis=0)

    def first_pass(v):
        def step(b, acc):
            at = pl.ds(pl.multiple_of(b * LANES, LANES), LANES)
            score = jnp.dot(units[v, at, :], centers_ref[...], preferred_element_type=jnp.float32)
            scores[v, at, :] = score
            den = jnp.zeros((LANES, LANES), jnp.float32)
            out = []
            for t in range(tiles):
                soft = jnp.exp(score[:, lane(t)] * (1.0 / TEMP_PRED))
                if (t + 1) * LANES > width:
                    soft = jnp.where(valid[:, lane(t)], soft, 0.0)
                code = soft * soft
                codes[v, at, lane(t)] = code
                den = den + soft
                out.append(acc[t] + fold8(code))
            last_out[v, 2, pl.ds(b, 1), :] = fold_rows(den)
            return tuple(out)

        zero = tuple(jnp.zeros((8, LANES), jnp.float32) for _ in range(tiles))
        return to_sublanes(lax.fori_loop(0, blocks, step, zero))

    def column_pass(v):
        def step(b, acc):
            at = pl.ds(pl.multiple_of(b * LANES, LANES), LANES)
            weight = jnp.broadcast_to(row_scale[v, pl.ds(b, 1), :], (LANES, LANES)).T
            return tuple(acc[t] + fold8(codes[v, at, lane(t)] * weight) for t in range(tiles))

        zero = tuple(jnp.zeros((8, LANES), jnp.float32) for _ in range(tiles))
        return to_sublanes(lax.fori_loop(0, blocks, step, zero))

    def row_pass(v, scale, put):
        def step(b, carry):
            at = pl.ds(pl.multiple_of(b * LANES, LANES), LANES)
            acc = jnp.zeros((LANES, LANES), jnp.float32)
            for t in range(tiles):
                acc = acc + codes[v, at, lane(t)] * scale[:, lane(t)]
            put[pl.ds(b, 1), :] = fold_rows(acc)
            return carry

        lax.fori_loop(0, blocks, step, 0)

    def last_pass(v, scale):
        def step(b, carry):
            at = pl.ds(pl.multiple_of(b * LANES, LANES), LANES)
            mass = jnp.zeros((LANES, LANES), jnp.float32)
            cross = jnp.zeros((LANES, LANES), jnp.float32)
            for t in range(tiles):
                raw = codes[v, at, lane(t)] * scale[:, lane(t)]
                mass = mass + raw
                cross = cross + raw * scores[1 - v, at, lane(t)]
            last_out[v, 0, pl.ds(b, 1), :] = fold_rows(mass)
            last_out[v, 1, pl.ds(b, 1), :] = fold_rows(cross) * (1.0 / TEMP_PRED)
            return carry

        lax.fori_loop(0, blocks, step, 0)

    def send_columns(r, v, part):
        col_out[r, v] = part
        return [
            send(col_out.at[r, v], col_in.at[r, v, d], col_send.at[r, v, d], col_recv.at[r, v, d],
                 {"ba": ba_peer[d]})
            for d in range(1, nba)
        ]

    def send_samples(r, v):
        return [
            send(row_out.at[r, v], row_in.at[r, v, d], row_send.at[r, v, d], row_recv.at[r, v, d],
                 {"ka": ka_peer[d]})
            for d in range(1, nka)
        ]

    def column_scale(r, v, copies):
        total = col_out[r, v]
        for d in range(1, nba):
            copies[d - 1].wait_recv()
            total = total + col_in[r, v, d]
        return jnp.where(valid, 1.0 / total, 0.0)

    cols = [send_columns(0, v, first_pass(v)) for v in range(2)]
    for r in range(REPEAT_COUNT - 1):
        samples = []
        for v in range(2):
            row_pass(v, column_scale(r, v, cols[v]), row_out.at[r, v])
            samples.append(send_samples(r, v))
        cols = []
        for v in range(2):
            total = row_out[r, v]
            for d in range(1, nka):
                samples[v][d - 1].wait_recv()
                total = total + row_in[r, v, d]
            row_scale[v] = 1.0 / total
            cols.append(send_columns(r + 1, v, column_pass(v)))
    finals = []
    for v in range(2):
        scale = column_scale(REPEAT_COUNT - 1, v, cols[v])
        if v == 0:
            scale_ref[...] = scale
        last_pass(v, scale)
        finals.append([
            send(last_out.at[v], last_in.at[v, d], last_send.at[v, d], last_recv.at[v, d],
                 {"ka": ka_peer[d]})
            for d in range(1, nka)
        ])
    unit_ref[...] = units[0]
    loss = jnp.zeros(loss_ref.shape, jnp.float32)
    for v in range(2):
        mass, cross, den = last_out[v, 0], last_out[v, 1], last_out[v, 2]
        for d in range(1, nka):
            finals[v][d - 1].wait_recv()
            mass = mass + last_in[v, d, 0]
            cross = cross + last_in[v, d, 1]
            den = den + last_in[v, d, 2]
        if v == 0:
            mass_ref[...] = mass
        loss = loss + jnp.log(den) - cross / mass
    loss_ref[...] = loss
    for copy in pending:
        copy.wait_send()


def write_kernel(count, unit_ref, centers_ref, scale_ref, mass_ref, out_ref):
    step = pl.program_id(0)
    width = out_ref.shape[1]
    for b in range(out_ref.shape[0] // LANES):
        at = slice(b * LANES, (b + 1) * LANES)
        score = jnp.dot(unit_ref[at, :], centers_ref[...], preferred_element_type=jnp.float32)
        mass = mass_ref[pl.ds(step * (out_ref.shape[0] // LANES) + b, 1), :]
        weight = jnp.broadcast_to(count / mass, (LANES, LANES)).T
        for t in range(0, centers_ref.shape[1], LANES):
            end = min(t + LANES, width)
            soft = jnp.exp(score[:, t:end] * (1.0 / TEMP_PRED))
            out_ref[at, t:end] = soft * soft * scale_ref[:, t:end] * weight[:, : end - t]


def body(nba, nka, emb_one, emb_two, prototypes):
    rows, depth = emb_one.shape
    width, feat = prototypes.shape
    padded = -(-width // LANES) * LANES
    blocks = rows // LANES
    f32 = jnp.float32
    vmem = pl.BlockSpec(memory_space=pltpu.VMEM)
    dma = pltpu.SemaphoreType.DMA
    units, centers, scale, mass, loss = pl.pallas_call(
        functools.partial(balance_kernel, nba, nka, width),
        out_shape=(
            jax.ShapeDtypeStruct((rows, depth), jnp.bfloat16),
            jax.ShapeDtypeStruct((depth, padded), jnp.bfloat16),
            jax.ShapeDtypeStruct((1, padded), f32),
            jax.ShapeDtypeStruct((blocks, LANES), f32),
            jax.ShapeDtypeStruct((blocks, LANES), f32),
        ),
        in_specs=[vmem] * 3,
        out_specs=[vmem] * 5,
        scratch_shapes=[
            pltpu.VMEM((2, rows, depth), jnp.bfloat16),
            pltpu.VMEM((nba, feat, width), f32),
            pltpu.VMEM((2, rows, padded), f32),
            pltpu.VMEM((2, rows, padded), f32),
            pltpu.VMEM((8, LANES), f32),
            pltpu.VMEM((2, blocks, LANES), f32),
            pltpu.VMEM((REPEAT_COUNT, 2, 1, padded), f32),
            pltpu.VMEM((REPEAT_COUNT, 2, nba, 1, padded), f32),
            pltpu.VMEM((REPEAT_COUNT - 1, 2, blocks, LANES), f32),
            pltpu.VMEM((REPEAT_COUNT - 1, 2, nka, blocks, LANES), f32),
            pltpu.VMEM((2, 3, blocks, LANES), f32),
            pltpu.VMEM((2, nka, 3, blocks, LANES), f32),
            dma((nba,)), dma((nba,)),
            dma((REPEAT_COUNT, 2, nba)), dma((REPEAT_COUNT, 2, nba)),
            dma((REPEAT_COUNT - 1, 2, nka)), dma((REPEAT_COUNT - 1, 2, nka)),
            dma((2, nka)), dma((2, nka)),
        ],
        compiler_params=pltpu.CompilerParams(
            collective_id=0, has_side_effects=True, vmem_limit_bytes=VMEM_LIMIT
        ),
    )(emb_one, emb_two, prototypes.T)
    chunk = 2 * LANES if rows % (2 * LANES) == 0 else LANES
    weights = pl.pallas_call(
        functools.partial(write_kernel, float(width * nka)),
        grid=(rows // chunk,),
        out_shape=jax.ShapeDtypeStruct((rows, width), f32),
        in_specs=[
            pl.BlockSpec((chunk, depth), lambda i: (i, 0)),
            pl.BlockSpec((depth, padded), lambda i: (0, 0)),
            pl.BlockSpec((1, padded), lambda i: (0, 0)),
            pl.BlockSpec((blocks, LANES), lambda i: (0, 0)),
        ],
        out_specs=pl.BlockSpec((chunk, width), lambda i: (i, 0)),
    )(units, centers, scale, mass)
    return weights, loss.reshape(rows)


def solution(mesh):
    placed = (P("ba", None), P("ba", None), P("ka", "ba"))
    return jax.shard_map(
        functools.partial(body, mesh.shape["ba"], mesh.shape["ka"]),
        mesh=mesh, in_specs=placed, out_specs=(P("ba", "ka"), P("ba")), check_vma=False,
    )
```

```python
import functools

import jax
import jax.numpy as jnp
from jax import lax
from jax.experimental import pallas as pl
from jax.experimental.pallas import tpu as pltpu
from jax.sharding import PartitionSpec as P

REPEAT_COUNT = 3
TEMP_CODE = 0.05
TEMP_PRED = 0.1
LANES = 128
VMEM_LIMIT = 67_043_328
MESH = pl.DeviceIdType.MESH


def unit(values):
    values = values.astype(jnp.float32)
    return (values * lax.rsqrt(jnp.sum(values * values, axis=1, keepdims=True))).astype(jnp.bfloat16)


def fold_rows(tile):
    return jnp.sum(tile.T, axis=0, keepdims=True)


def balance_kernel(
    nba, nka, width,
    one_hbm, two_hbm, proto_hbm,
    unit_ref, centers_ref, scale_ref, mass_ref, loss_ref,
    one_ref, two_ref, proto_ref, units, gathered, scores, codes, row_scale, load_sem,
    col_out, col_in, row_out, row_in, last_out, last_in,
    gather_send, gather_recv, col_send, col_recv, row_send, row_recv, last_send, last_recv,
):
    mine_ba = lax.axis_index("ba")
    mine_ka = lax.axis_index("ka")
    rows = one_ref.shape[0]
    blocks = rows // LANES
    feat = proto_ref.shape[0]
    padded = centers_ref.shape[1]
    tiles = padded // LANES
    ba_peer = [lax.rem(mine_ba + d, nba) for d in range(nba)]
    ka_peer = [lax.rem(mine_ka + d, nka) for d in range(nka)]

    loads = [
        pltpu.make_async_copy(src, dst, load_sem.at[i])
        for i, (src, dst) in enumerate(((proto_hbm, proto_ref), (one_hbm, one_ref), (two_hbm, two_ref)))
    ]
    for load in loads:
        load.start()
    barrier = pltpu.get_barrier_semaphore()
    for d in range(1, nba):
        pl.semaphore_signal(barrier, inc=1, device_id={"ba": ba_peer[d]}, device_id_type=MESH)
    for d in range(1, nka):
        pl.semaphore_signal(barrier, inc=1, device_id={"ka": ka_peer[d]}, device_id_type=MESH)
    pl.semaphore_wait(barrier, nba + nka - 2)

    pending = []

    def send(src, dst, send_sem, recv_sem, peer):
        copy = pltpu.make_async_remote_copy(
            src_ref=src, dst_ref=dst, send_sem=send_sem, recv_sem=recv_sem,
            device_id=peer, device_id_type=MESH,
        )
        copy.start()
        pending.append(copy)
        return copy

    pair = 2 if nba % 2 == 0 else 1
    groups = nba // pair
    group, side = mine_ba // pair, lax.rem(mine_ba, pair)
    other = group * pair + (pair - 1 - side)
    loads[0].wait()
    gathers = [
        send(proto_ref, gathered.at[mine_ba], gather_send.at[d], gather_recv.at[d],
             {"ba": lax.rem(group + d, groups) * pair + side})
        for d in range(1, groups)
    ]
    crossed = []
    if pair == 2:
        crossed.append(send(proto_ref, gathered.at[mine_ba], gather_send.at[groups],
                            gather_recv.at[groups], {"ba": other}))
    gathered[mine_ba] = proto_ref[...]
    loads[1].wait()
    loads[2].wait()

    def norm_block(b, carry):
        at = pl.ds(pl.multiple_of(b * LANES, LANES), LANES)
        units[0, at, :] = unit(one_ref[at, :])
        units[1, at, :] = unit(two_ref[at, :])
        return carry

    order = sorted(range(1, groups), key=lambda d: min(d, groups - d))
    share = -(-blocks // max(len(order), 1))
    for place, d in enumerate(order):
        gathers[d - 1].wait_recv()
        if pair == 2:
            owner = lax.rem(group + (groups - d), groups) * pair + side
            crossed.append(send(gathered.at[owner], gathered.at[owner], gather_send.at[groups + d],
                                gather_recv.at[groups + d], {"ba": other}))
        lax.fori_loop(min(place * share, blocks), min((place + 1) * share, blocks), norm_block, 0)
    if not order:
        lax.fori_loop(0, blocks, norm_block, 0)
    for copy in crossed:
        copy.wait_recv()
    whole = jnp.concatenate([gathered[b] for b in range(nba)], axis=0)
    factor = lax.rsqrt(jnp.sum(whole * whole, axis=0, keepdims=True))
    centers_ref[...] = jnp.zeros_like(centers_ref)
    centers_ref[:, :width] = (whole * factor).astype(jnp.bfloat16)

    valid = lax.broadcasted_iota(jnp.int32, (1, padded), 1) < width

    def lane(t):
        return slice(t * LANES, (t + 1) * LANES)

    def to_sublanes(acc):
        return jnp.concatenate([jnp.sum(a, axis=0, keepdims=True) for a in acc], axis=1)

    def fold8(tile):
        return jnp.sum(tile.reshape(LANES // 8, 8, LANES), axis=0)

    def first_pass(v):
        def step(b, acc):
            at = pl.ds(pl.multiple_of(b * LANES, LANES), LANES)
            score = jnp.dot(units[v, at, :], centers_ref[...], preferred_element_type=jnp.float32)
            scores[v, at, :] = score
            den = jnp.zeros((LANES, LANES), jnp.float32)
            out = []
            for t in range(tiles):
                soft = jnp.exp(score[:, lane(t)] * (1.0 / TEMP_PRED))
                if (t + 1) * LANES > width:
                    soft = jnp.where(valid[:, lane(t)], soft, 0.0)
                code = soft * soft
                codes[v, at, lane(t)] = code
                den = den + soft
                out.append(acc[t] + fold8(code))
            last_out[v, 2, pl.ds(b, 1), :] = fold_rows(den)
            return tuple(out)

        zero = tuple(jnp.zeros((8, LANES), jnp.float32) for _ in range(tiles))
        return to_sublanes(lax.fori_loop(0, blocks, step, zero))

    def column_pass(v):
        def step(b, acc):
            at = pl.ds(pl.multiple_of(b * LANES, LANES), LANES)
            weight = jnp.broadcast_to(row_scale[v, pl.ds(b, 1), :], (LANES, LANES)).T
            return tuple(acc[t] + fold8(codes[v, at, lane(t)] * weight) for t in range(tiles))

        zero = tuple(jnp.zeros((8, LANES), jnp.float32) for _ in range(tiles))
        return to_sublanes(lax.fori_loop(0, blocks, step, zero))

    def row_pass(v, scale, put):
        def step(b, carry):
            at = pl.ds(pl.multiple_of(b * LANES, LANES), LANES)
            acc = jnp.zeros((LANES, LANES), jnp.float32)
            for t in range(tiles):
                acc = acc + codes[v, at, lane(t)] * scale[:, lane(t)]
            put[pl.ds(b, 1), :] = fold_rows(acc)
            return carry

        lax.fori_loop(0, blocks, step, 0)

    def last_pass(v, scale):
        def step(b, carry):
            at = pl.ds(pl.multiple_of(b * LANES, LANES), LANES)
            mass = jnp.zeros((LANES, LANES), jnp.float32)
            cross = jnp.zeros((LANES, LANES), jnp.float32)
            for t in range(tiles):
                raw = codes[v, at, lane(t)] * scale[:, lane(t)]
                mass = mass + raw
                cross = cross + raw * scores[1 - v, at, lane(t)]
            last_out[v, 0, pl.ds(b, 1), :] = fold_rows(mass)
            last_out[v, 1, pl.ds(b, 1), :] = fold_rows(cross) * (1.0 / TEMP_PRED)
            return carry

        lax.fori_loop(0, blocks, step, 0)

    def send_columns(r, v, part):
        col_out[r, v] = part
        return [
            send(col_out.at[r, v], col_in.at[r, v, d], col_send.at[r, v, d], col_recv.at[r, v, d],
                 {"ba": ba_peer[d]})
            for d in range(1, nba)
        ]

    def send_samples(r, v):
        return [
            send(row_out.at[r, v], row_in.at[r, v, d], row_send.at[r, v, d], row_recv.at[r, v, d],
                 {"ka": ka_peer[d]})
            for d in range(1, nka)
        ]

    def column_scale(r, v, copies):
        total = col_out[r, v]
        for d in range(1, nba):
            copies[d - 1].wait_recv()
            total = total + col_in[r, v, d]
        return jnp.where(valid, 1.0 / total, 0.0)

    cols = [send_columns(0, v, first_pass(v)) for v in range(2)]
    for r in range(REPEAT_COUNT - 1):
        samples = []
        for v in range(2):
            row_pass(v, column_scale(r, v, cols[v]), row_out.at[r, v])
            samples.append(send_samples(r, v))
        cols = []
        for v in range(2):
            total = row_out[r, v]
            for d in range(1, nka):
                samples[v][d - 1].wait_recv()
                total = total + row_in[r, v, d]
            row_scale[v] = 1.0 / total
            cols.append(send_columns(r + 1, v, column_pass(v)))
    finals = []
    for v in range(2):
        scale = column_scale(REPEAT_COUNT - 1, v, cols[v])
        if v == 0:
            scale_ref[...] = scale
        last_pass(v, scale)
        finals.append([
            send(last_out.at[v], last_in.at[v, d], last_send.at[v, d], last_recv.at[v, d],
                 {"ka": ka_peer[d]})
            for d in range(1, nka)
        ])
    unit_ref[...] = units[0]
    loss = jnp.zeros(loss_ref.shape, jnp.float32)
    for v in range(2):
        mass, cross, den = last_out[v, 0], last_out[v, 1], last_out[v, 2]
        for d in range(1, nka):
            finals[v][d - 1].wait_recv()
            mass = mass + last_in[v, d, 0]
            cross = cross + last_in[v, d, 1]
            den = den + last_in[v, d, 2]
        if v == 0:
            mass_ref[...] = mass
        loss = loss + jnp.log(den) - cross / mass
    loss_ref[...] = loss
    for copy in pending:
        copy.wait_send()


def write_kernel(
    count, unit_ref, centers_ref, scale_ref, mass_ref, loss_ref, out_hbm, loss_out, out_ref, sem
):
    width, rows = out_ref.shape
    copies = []
    for start in range(0, width, LANES):
        size = min(LANES, width - start)
        tile = slice(start, start + LANES)
        score = lax.dot_general(
            centers_ref[:, tile], unit_ref[...], (((0,), (1,)), ((), ())), preferred_element_type=jnp.float32
        )
        weight = jnp.broadcast_to(scale_ref[:, tile] * count, (LANES, LANES)).T
        for b in range(rows // LANES):
            at = slice(b * LANES, (b + 1) * LANES)
            soft = jnp.exp(score[:, at] * (1.0 / TEMP_PRED))
            value = soft * soft * weight * (1.0 / mass_ref[b : b + 1, :])
            out_ref[start : start + size, at] = value[:size]
        part = pl.ds(start, size)
        copies.append(pltpu.make_async_copy(out_ref.at[part], out_hbm.at[part], sem.at[len(copies)]))
        copies[-1].start()
    loss_out[...] = loss_ref[...]
    for copy in copies:
        copy.wait()


def body(nba, nka, emb_one, emb_two, prototypes):
    rows, depth = emb_one.shape
    width, feat = prototypes.shape
    padded = -(-width // LANES) * LANES
    blocks = rows // LANES
    f32 = jnp.float32
    vmem = pl.BlockSpec(memory_space=pltpu.VMEM)
    dma = pltpu.SemaphoreType.DMA
    units, centers, scale, mass, loss = pl.pallas_call(
        functools.partial(balance_kernel, nba, nka, width),
        out_shape=(
            jax.ShapeDtypeStruct((rows, depth), jnp.bfloat16),
            jax.ShapeDtypeStruct((depth, padded), jnp.bfloat16),
            jax.ShapeDtypeStruct((1, padded), f32),
            jax.ShapeDtypeStruct((blocks, LANES), f32),
            jax.ShapeDtypeStruct((blocks, LANES), f32),
        ),
        in_specs=[pl.BlockSpec(memory_space=pltpu.HBM)] * 3,
        out_specs=[vmem] * 5,
        scratch_shapes=[
            pltpu.VMEM((rows, depth), jnp.bfloat16),
            pltpu.VMEM((rows, depth), jnp.bfloat16),
            pltpu.VMEM((feat, width), f32),
            pltpu.VMEM((2, rows, depth), jnp.bfloat16),
            pltpu.VMEM((nba, feat, width), f32),
            pltpu.VMEM((2, rows, padded), f32),
            pltpu.VMEM((2, rows, padded), f32),
            pltpu.VMEM((2, blocks, LANES), f32),
            dma((3,)),
            pltpu.VMEM((REPEAT_COUNT, 2, 1, padded), f32),
            pltpu.VMEM((REPEAT_COUNT, 2, nba, 1, padded), f32),
            pltpu.VMEM((REPEAT_COUNT - 1, 2, blocks, LANES), f32),
            pltpu.VMEM((REPEAT_COUNT - 1, 2, nka, blocks, LANES), f32),
            pltpu.VMEM((2, 3, blocks, LANES), f32),
            pltpu.VMEM((2, nka, 3, blocks, LANES), f32),
            dma((nba,)), dma((nba,)),
            dma((REPEAT_COUNT, 2, nba)), dma((REPEAT_COUNT, 2, nba)),
            dma((REPEAT_COUNT - 1, 2, nka)), dma((REPEAT_COUNT - 1, 2, nka)),
            dma((2, nka)), dma((2, nka)),
        ],
        compiler_params=pltpu.CompilerParams(
            collective_id=0, has_side_effects=True, vmem_limit_bytes=VMEM_LIMIT
        ),
    )(emb_one, emb_two, prototypes.T)
    weights, loss = pl.pallas_call(
        functools.partial(write_kernel, float(width * nka)),
        out_shape=(
            jax.ShapeDtypeStruct((width, rows), f32),
            jax.ShapeDtypeStruct((blocks, LANES), f32),
        ),
        in_specs=[vmem] * 5,
        out_specs=(pl.BlockSpec(memory_space=pltpu.HBM), vmem),
        scratch_shapes=[pltpu.VMEM((width, rows), f32), dma((padded // LANES,))],
    )(units, centers, scale, mass, loss)
    return weights.T, loss.reshape(rows)


def solution(mesh):
    placed = (P("ba", None), P("ba", None), P("ka", "ba"))
    return jax.shard_map(
        functools.partial(body, mesh.shape["ba"], mesh.shape["ka"]),
        mesh=mesh, in_specs=placed, out_specs=(P("ba", "ka"), P("ba")), check_vma=False,
    )
```
